32 devices in a mesh: groups: 2 (over y), seq: 4 (over z), head: 2 (over x), rep: 2 (over core).
Axes of the slice: x: 2, y: 2, z: 4, core: 2. Of those that a mesh axis runs over, the one named last changes fastest.
Arguments:
- q_latent: bfloat16 [32, 2, 128, 512], P('groups', None, 'head'), parts along dimension 0, may hold values from -40 to 40
- q_rope: bfloat16 [32, 2, 128, 64], P('groups', None, 'head'), parts along dimension 0, may hold values from -40 to 40
- cache_latent: bfloat16 [32, 512, 512], P(('groups', 'rep'), 'seq'), parts along dimension 0, may hold values from -20 to 20
- rope_keys: bfloat16 [32, 64, 512], P(('groups', 'rep'), None, 'seq'), parts along dimension 0, may hold values from -20 to 20
- lengths: int32 [32], P(('groups', 'rep')), parts along dimension 0, may hold values from 128 to 512, as said below
- slot_request: int32 [32], P(('groups', 'rep')), parts along dimension 0, may hold values from 0 to 15, as said below
- value_up: bfloat16 [128, 512, 128], P('head'), may hold values from -0.25 to 0.25
Outputs:
- values: bfloat16 [32, 2, 128, 128], P(('groups', 'rep'), None, 'head'), parts along dimension 0
The draws below stay inside these ranges and needn't reach their ends.
There are 2 independent parts, one for each index of `groups`. The reference program is written for one: setup_inputs(seed, part) draws one part's arguments, and reference() takes and returns one part's arrays. A program takes and returns all parts, laid end to end along the dimension named above; an argument that names none is the same for every part. Nothing has to cross between parts.
Inputs may be any that keep to these rules, and one draw needn't show every extreme that they name: `lengths`: each slot's length lies between 128 and 512; in every part some slot holds 512. `slot_request`: a permutation of the requests 0 to 15.
All inputs are finite; a program needn't handle non-finite values.
Results may differ from the reference program's by a relative error of at most 0.0021.
Values may be sent and summed in bfloat16 or wider, within the bound.
A program may use at most 64 MiB of HBM per device.

```python
import jax
import jax.numpy as jnp
from jax import lax

HEADS = 128
LATENT = 512
ROPE = 64
NOPE = 128
DV = 128
QTOK = 2
PAGE = 128
BATCH = 16
SEQ_LEN = 512


def slot_order(key):
    return jax.random.permutation(jax.random.fold_in(key, 11), BATCH).astype(jnp.int32)


def cache_parts(key):
    latent = jax.random.truncated_normal(jax.random.fold_in(key, 12), -5.0, 5.0, (BATCH, SEQ_LEN, LATENT), jnp.float32)
    rotary = jax.random.truncated_normal(jax.random.fold_in(key, 13), -5.0, 5.0, (BATCH, ROPE, SEQ_LEN), jnp.float32)
    return (latent, rotary)


def shared_queries(key):
    lat_shape = (BATCH, QTOK, HEADS, LATENT)
    rot_shape = (BATCH, QTOK, HEADS, ROPE)
    query_lat = 2.0 * jax.random.truncated_normal(jax.random.fold_in(key, 21), -5.0, 5.0, lat_shape, jnp.float32)
    query_rot = 2.0 * jax.random.truncated_normal(jax.random.fold_in(key, 22), -5.0, 5.0, rot_shape, jnp.float32)
    return (query_lat, query_rot)


def draw_q_latent(key, part):
    return shared_queries(key)[0].astype(jnp.bfloat16)


def draw_q_rope(key, part):
    return shared_queries(key)[1].astype(jnp.bfloat16)


def draw_cache_latent(key, part):
    return cache_parts(key)[0].astype(jnp.bfloat16)


def draw_rope_keys(key, part):
    return cache_parts(key)[1].astype(jnp.bfloat16)


def draw_lengths(key, part):
    drawn = jax.random.randint(jax.random.fold_in(key, 31), (BATCH,), PAGE, SEQ_LEN + 1)
    longest = jax.random.randint(jax.random.fold_in(key, 32), (), 0, BATCH)
    return drawn.at[longest].set(SEQ_LEN).astype(jnp.int32)


def draw_slot_request(key, part):
    return slot_order(key)


def level_of(key, dims, pieces, least, top_value):
    level = 1.0
    for dim, parts in pieces:
        heights = jax.random.uniform(jax.random.fold_in(jax.random.fold_in(key, 6), dim), (parts,), jnp.float32, least / len(pieces), top_value / len(pieces))
        level = level * jnp.repeat(jnp.exp(heights), dims[dim] // parts).reshape((-1,) + (1,) * (len(dims) - 1 - dim))
    return level


def gaussian(rng, shape, width, bound, cuts=(), kind=jnp.bfloat16):
    values = width * jax.random.normal(rng, shape, jnp.float32)
    if cuts:
        values = values * level_of(rng, shape, cuts, -0.22, 0.18)
    return jnp.clip(values, -bound, bound).astype(kind)


def setup_inputs(seed: int = 0, part: int = 0) -> dict:
    streams_of = jax.random.split(jax.random.key(seed), 8)
    part_keys = jax.random.split(jax.random.fold_in(streams_of[7], part), 8)
    return {
        "q_latent": draw_q_latent(jax.random.fold_in(jax.random.fold_in(streams_of[7], part), 71), part),
        "q_rope": draw_q_rope(jax.random.fold_in(jax.random.fold_in(streams_of[7], part), 71), part),
        "cache_latent": draw_cache_latent(jax.random.fold_in(jax.random.fold_in(streams_of[7], part), 71), part),
        "rope_keys": draw_rope_keys(jax.random.fold_in(jax.random.fold_in(streams_of[7], part), 71), part),
        "lengths": draw_lengths(jax.random.fold_in(jax.random.fold_in(streams_of[7], part), 71), part),
        "slot_request": draw_slot_request(jax.random.fold_in(jax.random.fold_in(streams_of[7], part), 71), part),
        "value_up": gaussian(streams_of[6], (HEADS, LATENT, DV), LATENT ** -0.5, 0.25, ((0, 2),)),
    }


negative_fill = -1e30


def reference(q_latent, q_rope, cache_latent, rope_keys, lengths, slot_request, value_up):
    softmax_scale = (NOPE + ROPE) ** -0.5
    page_count = SEQ_LEN // PAGE
    weight = value_up.astype(jnp.float32)

    def per_slot(slot_index):
        request = slot_request[slot_index]
        query_lat = q_latent[request].astype(jnp.float32)
        query_rot = q_rope[request].astype(jnp.float32)
        cache_rows = cache_latent[slot_index].astype(jnp.float32)
        rope_rows = rope_keys[slot_index].astype(jnp.float32)
        scores = jnp.einsum("thd,pd->thp", query_lat, cache_rows)
        scores = (scores + jnp.einsum("the,ep->thp", query_rot, rope_rows)) * softmax_scale
        positions = jnp.arange(SEQ_LEN, dtype=jnp.int32)
        limits = lengths[slot_index] - QTOK + 1 + jnp.arange(QTOK, dtype=jnp.int32)
        visible = positions[None, :] < limits[:, None]
        visible = jnp.broadcast_to(visible[:, None, :], scores.shape).reshape(QTOK, HEADS, page_count, PAGE)
        masked = jnp.where(visible, scores.reshape(QTOK, HEADS, page_count, PAGE), negative_fill)
        page_max = jnp.max(masked, axis=3)
        page_exp = jnp.where(visible, jnp.exp(masked - page_max[..., None]), 0.0)
        page_den = jnp.sum(page_exp, axis=3)
        page_weights = lax.optimization_barrier(page_exp.astype(jnp.bfloat16)).astype(jnp.float32)
        page_out = jnp.einsum("thnp,npd->thnd", page_weights, cache_rows.reshape(page_count, PAGE, LATENT))
        largest = jnp.max(page_max, axis=2)
        factor = jnp.exp(page_max - largest[..., None])
        denominator = jnp.sum(factor * page_den, axis=2)
        summed = jnp.sum(factor[..., None] * page_out, axis=2)
        attended = summed / denominator[..., None]
        result = jnp.einsum("thd,hdv->thv", attended, weight, precision=lax.Precision.HIGHEST)
        return result.astype(jnp.bfloat16)

    return lax.map(per_slot, jnp.arange(BATCH, dtype=jnp.int32))
```

```python
import functools

import jax
import jax.numpy as jnp
from jax import lax
from jax.experimental import pallas as pl
from jax.experimental.pallas import tpu as pltpu
from jax.sharding import PartitionSpec as P

ROPE = 64
NOPE = 128
MESH = pl.DeviceIdType.MESH
LANES = 128


negative_fill = -1e30


def kernel(n, lengths_ref, request_ref, qlat_hbm, qrot_hbm, cache_hbm, rope_hbm, w_hbm, out_ref,
           qlat, qrot, cache, rope, w, weights, x, own, stat_out, stat_in, send, recv,
           load_sem, w_sem, stat_ssem, stat_rsem, rs_ssem, rs_rsem, ag_ssem, ag_rsem):
    slots, page, latent = cache.shape
    toks, heads = qlat.shape[1], qlat.shape[2]
    rows = toks * heads
    group = toks * slots
    per = heads // n
    me = lax.axis_index("seq")
    order = sorted(range(1, n), key=lambda k: abs(k - n / 2)) + [0]

    def peer(k):
        return lax.rem(me + k, n)

    loads = [
        pltpu.make_async_copy(src, dst, load_sem.at[i])
        for i, (src, dst) in enumerate(
            ((qlat_hbm, qlat), (cache_hbm, cache), (qrot_hbm, qrot), (rope_hbm, rope)))
    ]
    for copy in loads:
        copy.start()

    def w_load(k):
        part = pl.ds(peer(k) * per, per)
        return pltpu.make_async_copy(w_hbm.at[part], w.at[part], w_sem.at[k])

    for k in order:
        w_load(k).start()

    barrier = pltpu.get_barrier_semaphore()
    for k in range(1, n):
        pl.semaphore_signal(barrier, inc=1, device_id={"seq": peer(k)}, device_id_type=MESH)

    for copy in loads:
        copy.wait()

    softmax_scale = (NOPE + ROPE) ** (-0.5)
    lane = lax.broadcasted_iota(jnp.int32, (rows, LANES), 1)
    token = lax.broadcasted_iota(jnp.int32, (rows, page), 0) // heads
    position = me * page + lax.broadcasted_iota(jnp.int32, (rows, page), 1)
    stat = jnp.zeros((rows, LANES), jnp.float32)
    for b in range(slots):
        r = request_ref[b]
        ql = qlat[r].reshape(rows, latent)
        qr = qrot[r].reshape(rows, qrot.shape[3])
        s = lax.dot_general(ql, cache[b], (((1,), (1,)), ((), ())), preferred_element_type=jnp.float32)
        s = s + jnp.dot(qr, rope[b], preferred_element_type=jnp.float32)
        s = s * softmax_scale
        visible = position < lengths_ref[b] - toks + 1 + token
        masked = jnp.where(visible, s, negative_fill)
        top = jnp.max(masked, axis=1, keepdims=True)
        e = jnp.where(visible, jnp.exp(masked - top), 0.0)
        den = jnp.sum(e, axis=1, keepdims=True)
        stat = jnp.where(lane == b, top, stat)
        stat = jnp.where(lane == slots + b, den, stat)
        weights[b] = e.astype(jnp.bfloat16)
    width = stat_out.shape[1]
    if rows < width:
        stat = jnp.concatenate([stat, jnp.zeros((width - rows, LANES), jnp.float32)], axis=0)
    mine = jnp.transpose(stat)[: 2 * slots]
    stat_out[...] = mine

    pl.semaphore_wait(barrier, n - 1)

    def stat_copy(k):
        return pltpu.make_async_remote_copy(
            src_ref=stat_out, dst_ref=stat_in.at[k], send_sem=stat_ssem.at[k], recv_sem=stat_rsem.at[k],
            device_id={"seq": peer(k)}, device_id_type=MESH)

    def rs_copy(k):
        return pltpu.make_async_remote_copy(
            src_ref=send.at[k], dst_ref=recv.at[k], send_sem=rs_ssem.at[k], recv_sem=rs_rsem.at[k],
            device_id={"seq": peer(k)}, device_id_type=MESH)

    def ag_copy(k):
        part = out_ref.at[pl.ds(me * per, per)]
        return pltpu.make_async_remote_copy(
            src_ref=part, dst_ref=part, send_sem=ag_ssem.at[k], recv_sem=ag_rsem.at[k],
            device_id={"seq": peer(k)}, device_id_type=MESH)

    for k in order[:-1]:
        stat_copy(k).start()

    for b in range(slots):
        po = jnp.dot(weights[b], cache[b], preferred_element_type=jnp.float32)
        for t in range(toks):
            for c in range(latent // LANES):
                x[c, pl.ds(t * slots + b, heads, stride=group), :] = (
                    po[t * heads:(t + 1) * heads, c * LANES:(c + 1) * LANES])

    for k in range(1, n):
        stat_copy(k).wait_recv()
    tops = [mine[:slots]] + [stat_in[k, :slots, :] for k in range(1, n)]
    dens = [mine[slots:]] + [stat_in[k, slots:, :] for k in range(1, n)]
    largest = functools.reduce(jnp.maximum, tops)
    total = functools.reduce(lambda a, b: a + b, [jnp.exp(t - largest) * d for t, d in zip(tops, dens)])
    coef = jnp.exp(tops[0] - largest) / total
    coef = jnp.concatenate(
        [coef if t == 0 else pltpu.roll(coef, width - t * heads, 1) for t in range(toks)], axis=0)

    for k in order:
        w_load(k).wait()
        dest = peer(k)
        turned = pltpu.roll(coef, lax.rem(width - dest * per, width), 1)
        parts = []
        for j in range(per):
            h = dest * per + j
            base = pl.multiple_of(h * group, group)
            xs = jnp.concatenate([x[c, pl.ds(base, group), :] for c in range(latent // LANES)], axis=1)
            hi = xs.astype(jnp.bfloat16)
            lo = (xs - hi.astype(jnp.float32)).astype(jnp.bfloat16)
            both = jnp.dot(jnp.concatenate([hi, lo], axis=0), w[h], preferred_element_type=jnp.float32)
            parts.append((both[:group] + both[group:]) * turned[:, j:j + 1])
        if k == 0:
            for j in range(per):
                own[j] = parts[j]
        else:
            for j in range(per):
                send[k, j] = parts[j]
            rs_copy(k).start()

    for k in order[:-1]:
        rs_copy(k).wait_recv()
    for j in range(per):
        acc = own[j]
        for k in range(1, n):
            acc = acc + recv[k, j]
        out_ref[me * per + j] = acc.astype(jnp.bfloat16)
    for k in order[:-1]:
        ag_copy(k).start()
    for k in order[:-1]:
        stat_copy(k).wait_send()
        rs_copy(k).wait_send()
    for k in order[:-1]:
        ag_copy(k).wait()


def per_device(n, q_latent, q_rope, cache_latent, rope_keys, lengths, slot_request, value_up):
    toks, heads = q_latent.shape[1], q_latent.shape[2]
    slots, page, latent = cache_latent.shape
    dv = value_up.shape[2]
    group = toks * slots
    per = heads // n
    rows = toks * heads
    width = -(-rows // LANES) * LANES
    hbm = pl.BlockSpec(memory_space=pltpu.HBM)
    smem = pl.BlockSpec(memory_space=pltpu.SMEM)
    dma = pltpu.SemaphoreType.DMA
    out = pl.pallas_call(
        functools.partial(kernel, n),
        out_shape=jax.ShapeDtypeStruct((heads, group, dv), jnp.bfloat16),
        in_specs=[smem, smem, hbm, hbm, hbm, hbm, hbm],
        out_specs=pl.BlockSpec(memory_space=pltpu.VMEM),
        scratch_shapes=[
            pltpu.VMEM(q_latent.shape, jnp.bfloat16),
            pltpu.VMEM(q_rope.shape, jnp.bfloat16),
            pltpu.VMEM(cache_latent.shape, jnp.bfloat16),
            pltpu.VMEM(rope_keys.shape, jnp.bfloat16),
            pltpu.VMEM(value_up.shape, jnp.bfloat16),
            pltpu.VMEM((slots, rows, page), jnp.bfloat16),
            pltpu.VMEM((latent // LANES, heads * group, LANES), jnp.float32),
            pltpu.VMEM((per, group, dv), jnp.float32),
            pltpu.VMEM((2 * slots, width), jnp.float32),
            pltpu.VMEM((n, 2 * slots, width), jnp.float32),
            pltpu.VMEM((n, per, group, dv), jnp.float32),
            pltpu.VMEM((n, per, group, dv), jnp.float32),
            dma((4,)), dma((n,)), dma((n,)), dma((n,)), dma((n,)), dma((n,)),
            dma((n,)), dma((n,)),
        ],
        compiler_params=pltpu.CompilerParams(
            collective_id=0, has_side_effects=True, vmem_limit_bytes=67043328),
    )(lengths, slot_request, q_latent, q_rope, cache_latent, rope_keys, value_up)
    return jnp.transpose(out.reshape(heads, toks, slots, dv), (2, 1, 0, 3))


def solution(mesh):
    in_specs = (
        P("groups", None, "head", None),
        P("groups", None, "head", None),
        P(("groups", "rep"), "seq", None),
        P(("groups", "rep"), None, "seq"),
        P(("groups", "rep")),
        P(("groups", "rep")),
        P("head", None, None),
    )
    out_specs = P(("groups", "rep"), None, "head", None)
    return jax.shard_map(
        functools.partial(per_device, mesh.shape["seq"]),
        mesh=mesh, in_specs=in_specs, out_specs=out_specs, check_vma=False,
    )
```

```python
import functools

import jax
import jax.numpy as jnp
from jax import lax
from jax.experimental import pallas as pl
from jax.experimental.pallas import tpu as pltpu
from jax.sharding import PartitionSpec as P

ROPE = 64
NOPE = 128
MESH = pl.DeviceIdType.MESH
LANES = 128
CUTS = 2
CODE = 32767.0


negative_fill = -1e30


def kernel(n, cuts, lengths_ref, request_ref, qlat_hbm, qrot_hbm, cache_hbm, rope_hbm, w_hbm, out_ref,
           qlat, qrot, cache, rope, w, weights, x, own, stat_out, stat_in, send, recv, scale_out, scale_in,
           load_sem, w_sem, stat_ssem, stat_rsem, rs_ssem, rs_rsem, sc_ssem, sc_rsem, ag_ssem, ag_rsem):
    slots, page, latent = cache.shape
    toks, heads = qlat.shape[1], qlat.shape[2]
    rows = toks * heads
    group = toks * slots
    per = heads // n
    cut = per // cuts
    me = lax.axis_index("seq")
    order = sorted(range(1, n), key=lambda k: abs(k - n / 2))
    steps = [(c, k) for c in range(cuts) for k in order] + [(c, 0) for c in range(cuts)]

    def peer(k):
        return lax.rem(me + k, n)

    loads = [
        pltpu.make_async_copy(src, dst, load_sem.at[i])
        for i, (src, dst) in enumerate(
            ((qlat_hbm, qlat), (cache_hbm, cache), (qrot_hbm, qrot), (rope_hbm, rope)))
    ]
    for copy in loads:
        copy.start()

    def w_load(c, k):
        part = pl.ds(peer(k) * per + c * cut, cut)
        return pltpu.make_async_copy(w_hbm.at[part], w.at[part], w_sem.at[c, k])

    for c, k in steps:
        w_load(c, k).start()

    barrier = pltpu.get_barrier_semaphore()
    for k in order:
        pl.semaphore_signal(barrier, inc=1, device_id={"seq": peer(k)}, device_id_type=MESH)

    for copy in loads:
        copy.wait()

    softmax_scale = (NOPE + ROPE) ** (-0.5)
    lane = lax.broadcasted_iota(jnp.int32, (rows, LANES), 1)
    token = lax.broadcasted_iota(jnp.int32, (rows, page), 0) // heads
    position = me * page + lax.broadcasted_iota(jnp.int32, (rows, page), 1)
    stat = jnp.zeros((rows, LANES), jnp.float32)
    for b in range(slots):
        r = request_ref[b]
        ql = qlat[r].reshape(rows, latent)
        qr = qrot[r].reshape(rows, qrot.shape[3])
        s = lax.dot_general(ql, cache[b], (((1,), (1,)), ((), ())), preferred_element_type=jnp.float32)
        s = s + jnp.dot(qr, rope[b], preferred_element_type=jnp.float32)
        s = s * softmax_scale
        visible = position < lengths_ref[b] - toks + 1 + token
        masked = jnp.where(visible, s, negative_fill)
        top = jnp.max(masked, axis=1, keepdims=True)
        e = jnp.where(visible, jnp.exp(masked - top), 0.0)
        den = jnp.sum(e, axis=1, keepdims=True)
        stat = jnp.where(lane == b, top, stat)
        stat = jnp.where(lane == slots + b, den, stat)
        weights[b] = e.astype(jnp.bfloat16)
    width = stat_out.shape[1]
    if rows < width:
        stat = jnp.concatenate([stat, jnp.zeros((width - rows, LANES), jnp.float32)], axis=0)
    mine = jnp.transpose(stat)[: 2 * slots]
    stat_out[...] = mine

    def remote(src, dst, ssem, rsem, k):
        return pltpu.make_async_remote_copy(
            src_ref=src, dst_ref=dst, send_sem=ssem, recv_sem=rsem,
            device_id={"seq": peer(k)}, device_id_type=MESH)

    def stat_copy(k):
        return remote(stat_out, stat_in.at[k], stat_ssem.at[k], stat_rsem.at[k], k)

    def rs_copy(c, k):
        return remote(send.at[c, k], recv.at[c, k], rs_ssem.at[c, k], rs_rsem.at[c, k], k)

    def sc_copy(c, k):
        return remote(scale_out.at[c, k], scale_in.at[c, k], sc_ssem.at[c, k], sc_rsem.at[c, k], k)

    def ag_copy(c, k):
        part = out_ref.at[pl.ds(me * per + c * cut, cut)]
        return remote(part, part, ag_ssem.at[c, k], ag_rsem.at[c, k], k)

    for b in range(slots):
        po = jnp.dot(weights[b], cache[b], preferred_element_type=jnp.float32)
        for t in range(toks):
            for i in range(latent // LANES):
                x[i, pl.ds(t * slots + b, heads, stride=group), :] = (
                    po[t * heads:(t + 1) * heads, i * LANES:(i + 1) * LANES])

    scale_lane = lax.broadcasted_iota(jnp.int32, scale_out.shape[2:], 1)
    for number, (c, k) in enumerate(steps):
        w_load(c, k).wait()
        scale = jnp.zeros(scale_out.shape[2:], jnp.float32)
        for j in range(cut):
            h = peer(k) * per + c * cut + j
            base = pl.multiple_of(h * group, group)
            xs = jnp.concatenate([x[i, pl.ds(base, group), :] for i in range(latent // LANES)], axis=1)
            hi = xs.astype(jnp.bfloat16)
            lo = (xs - hi.astype(jnp.float32)).astype(jnp.bfloat16)
            both = jnp.dot(jnp.concatenate([hi, lo], axis=0), w[h], preferred_element_type=jnp.float32)
            part = both[:group] + both[group:]
            if k == 0:
                own[c * cut + j] = part
            else:
                peak = jnp.maximum(jnp.max(jnp.abs(part), axis=1, keepdims=True), 1e-30)
                send[c, k, j] = jnp.round(part * (CODE / peak)).astype(jnp.int32).astype(jnp.int16)
                for t in range(toks):
                    scale = jnp.where(scale_lane == t * cut + j, peak[t * slots:(t + 1) * slots], scale)
        if k != 0:
            scale_out[c, k] = scale * (1.0 / CODE)
            if number == 0:
                pl.semaphore_wait(barrier, n - 1)
                for other in order:
                    stat_copy(other).start()
            sc_copy(c, k).start()
            rs_copy(c, k).start()

    for k in order:
        stat_copy(k).wait_recv()
    tops = [mine[:slots]] + [stat_in[k, :slots, :] for k in range(1, n)]
    dens = [mine[slots:]] + [stat_in[k, slots:, :] for k in range(1, n)]
    largest = functools.reduce(jnp.maximum, tops)
    factors = [jnp.exp(t - largest) for t in tops]
    total = functools.reduce(lambda a, b: a + b, [f * d for f, d in zip(factors, dens)])

    for c in range(cuts):
        for k in order:
            sc_copy(c, k).wait_recv()
            rs_copy(c, k).wait_recv()
        coefs = []
        for k in range(n):
            ratio = factors[k] / total
            halves = []
            for t in range(toks):
                shift = lax.rem(2 * width - t * heads - me * per - c * cut, width)
                turned = pltpu.roll(ratio, shift, 1)
                if k:
                    scale = scale_in[c, k]
                    turned = turned * (pltpu.roll(scale, width - t * cut, 1) if t else scale)
                halves.append(turned)
            coefs.append(jnp.concatenate(halves, axis=0))
        for j in range(cut):
            acc = own[c * cut + j] * coefs[0][:, j:j + 1]
            for k in range(1, n):
                acc = acc + recv[c, k, j].astype(jnp.float32) * coefs[k][:, j:j + 1]
            out_ref[me * per + c * cut + j] = acc.astype(jnp.bfloat16)
        for k in order:
            ag_copy(c, k).start()
    for k in order:
        stat_copy(k).wait_send()
        for c in range(cuts):
            sc_copy(c, k).wait_send()
            rs_copy(c, k).wait_send()
    for c in range(cuts):
        for k in order:
            ag_copy(c, k).wait()


def per_device(n, q_latent, q_rope, cache_latent, rope_keys, lengths, slot_request, value_up):
    toks, heads = q_latent.shape[1], q_latent.shape[2]
    slots, page, latent = cache_latent.shape
    dv = value_up.shape[2]
    group = toks * slots
    per = heads // n
    cuts = CUTS if per % (4 * CUTS) == 0 else 1
    cut = per // cuts
    rows = toks * heads
    width = -(-rows // LANES) * LANES
    hbm = pl.BlockSpec(memory_space=pltpu.HBM)
    smem = pl.BlockSpec(memory_space=pltpu.SMEM)
    dma = pltpu.SemaphoreType.DMA
    out = pl.pallas_call(
        functools.partial(kernel, n, cuts),
        out_shape=jax.ShapeDtypeStruct((heads, group, dv), jnp.bfloat16),
        in_specs=[smem, smem, hbm, hbm, hbm, hbm, hbm],
        out_specs=pl.BlockSpec(memory_space=pltpu.VMEM),
        scratch_shapes=[
            pltpu.VMEM(q_latent.shape, jnp.bfloat16),
            pltpu.VMEM(q_rope.shape, jnp.bfloat16),
            pltpu.VMEM(cache_latent.shape, jnp.bfloat16),
            pltpu.VMEM(rope_keys.shape, jnp.bfloat16),
            pltpu.VMEM(value_up.shape, jnp.bfloat16),
            pltpu.VMEM((slots, rows, page), jnp.bfloat16),
            pltpu.VMEM((latent // LANES, heads * group, LANES), jnp.float32),
            pltpu.VMEM((per, group, dv), jnp.float32),
            pltpu.VMEM((2 * slots, width), jnp.float32),
            pltpu.VMEM((n, 2 * slots, width), jnp.float32),
            pltpu.VMEM((cuts, n, cut, group, dv), jnp.int16),
            pltpu.VMEM((cuts, n, cut, group, dv), jnp.int16),
            pltpu.VMEM((cuts, n, slots, width), jnp.float32),
            pltpu.VMEM((cuts, n, slots, width), jnp.float32),
            dma((4,)), dma((cuts, n)), dma((n,)), dma((n,)),
            dma((cuts, n)), dma((cuts, n)), dma((cuts, n)), dma((cuts, n)), dma((cuts, n)), dma((cuts, n)),
        ],
        compiler_params=pltpu.CompilerParams(
            collective_id=0, has_side_effects=True, vmem_limit_bytes=67043328),
    )(lengths, slot_request, q_latent, q_rope, cache_latent, rope_keys, value_up)
    return jnp.transpose(out.reshape(heads, toks, slots, dv), (2, 1, 0, 3))


def solution(mesh):
    in_specs = (
        P("groups", None, "head", None),
        P("groups", None, "head", None),
        P(("groups", "rep"), "seq", None),
        P(("groups", "rep"), None, "seq"),
        P(("groups", "rep")),
        P(("groups", "rep")),
        P("head", None, None),
    )
    out_specs = P(("groups", "rep"), None, "head", None)
    return jax.shard_map(
        functools.partial(per_device, mesh.shape["seq"]),
        mesh=mesh, in_specs=in_specs, out_specs=out_specs, check_vma=False,
    )
```

```python
import functools

import jax
import jax.numpy as jnp
from jax import lax
from jax.experimental import pallas as pl
from jax.experimental.pallas import tpu as pltpu
from jax.sharding import PartitionSpec as P

ROPE = 64
NOPE = 128
MESH = pl.DeviceIdType.MESH
LANES = 128
CODE = 32767.0


negative_fill = -1e30


def kernel(n, lengths_ref, request_ref, qlat_hbm, qrot_hbm, cache_hbm, rope_hbm, w_hbm, out_ref,
           qlat, qrot, cache, rope, w, weights, x, own, turned, send, recv, meta_out, meta_in,
           load_sem, w_sem, rs_ssem, rs_rsem, meta_ssem, meta_rsem, ag_ssem, ag_rsem):
    slots, page, latent = cache.shape
    toks, heads = qlat.shape[1], qlat.shape[2]
    rows = toks * heads
    group = toks * slots
    per = heads // n
    direct = per % 16 == 0
    me = lax.axis_index("seq")
    order = [3, 2, 1] if n == 4 else list(range(1, n))

    def peer(k):
        if n == 4:
            return (me, me + 1 - 2 * lax.rem(me, 2), lax.rem(me + 2, 4), 3 - me)[k]
        return lax.rem(me + k, n)

    loads = [
        pltpu.make_async_copy(src, dst, load_sem.at[i])
        for i, (src, dst) in enumerate(
            ((qlat_hbm, qlat), (cache_hbm, cache), (qrot_hbm, qrot), (rope_hbm, rope)))
    ]
    for copy in loads:
        copy.start()

    def w_load(k):
        part = pl.ds(peer(k) * per, per)
        return pltpu.make_async_copy(w_hbm.at[part], w.at[part], w_sem.at[k])

    barrier = pltpu.get_barrier_semaphore()
    for k in order:
        pl.semaphore_signal(barrier, inc=1, device_id={"seq": peer(k)}, device_id_type=MESH)

    for copy in loads:
        copy.wait()
    for k in order + [0]:
        w_load(k).start()

    softmax_scale = (NOPE + ROPE) ** (-0.5)
    lane = lax.broadcasted_iota(jnp.int32, (rows, LANES), 1)
    token = lax.broadcasted_iota(jnp.int32, (rows, page), 0) // heads
    position = me * page + lax.broadcasted_iota(jnp.int32, (rows, page), 1)
    stat = jnp.zeros((rows, LANES), jnp.float32)
    for b in range(slots):
        r = request_ref[b]
        ql = qlat[r].reshape(rows, latent)
        qr = qrot[r].reshape(rows, qrot.shape[3])
        s = lax.dot_general(ql, cache[b], (((1,), (1,)), ((), ())), preferred_element_type=jnp.float32)
        s = s + jnp.dot(qr, rope[b], preferred_element_type=jnp.float32)
        s = s * softmax_scale
        visible = position < lengths_ref[b] - toks + 1 + token
        masked = jnp.where(visible, s, negative_fill)
        top = jnp.max(masked, axis=1, keepdims=True)
        e = jnp.where(visible, jnp.exp(masked - top), 0.0)
        den = jnp.sum(e, axis=1, keepdims=True)
        stat = jnp.where(lane == b, top, stat)
        stat = jnp.where(lane == slots + b, den, stat)
        weights[b] = e.astype(jnp.bfloat16)
    width = meta_out.shape[3]
    if rows < width:
        stat = jnp.concatenate([stat, jnp.zeros((width - rows, LANES), jnp.float32)], axis=0)
    mine = jnp.transpose(stat)[: 2 * slots]
    meta_lane = lax.broadcasted_iota(jnp.int32, (2 * slots, width), 1)
    scale_lane = meta_lane[:slots]

    def stats_of(dest):
        picked = mine
        for t in range(toks):
            shift = lax.rem(2 * width - t * (heads - per) - dest * per, width)
            moved = pltpu.roll(mine, shift, 1)
            picked = moved if t == 0 else jnp.where(meta_lane >= t * per, moved, picked)
        return picked[:slots], picked[slots:]

    def remote(src, dst, ssem, rsem, k):
        return pltpu.make_async_remote_copy(
            src_ref=src, dst_ref=dst, send_sem=ssem, recv_sem=rsem,
            device_id={"seq": peer(k)}, device_id_type=MESH)

    def rs_copy(k):
        return remote(send.at[k], recv.at[k], rs_ssem.at[k], rs_rsem.at[k], k)

    def meta_copy(k):
        return remote(meta_out.at[k], meta_in.at[k], meta_ssem.at[k], meta_rsem.at[k], k)

    def ag_copy(k):
        part = pl.ds(me * per, per)
        part = out_ref.at[:, part] if direct else out_ref.at[part]
        return remote(part, part, ag_ssem.at[k], ag_rsem.at[k], k)

    for b in range(slots):
        po = jnp.dot(weights[b], cache[b], preferred_element_type=jnp.float32)
        for t in range(toks):
            for i in range(latent // LANES):
                x[i, pl.ds(t * slots + b, heads, stride=group), :] = (
                    po[t * heads:(t + 1) * heads, i * LANES:(i + 1) * LANES])

    for k in order + [0]:
        w_load(k).wait()
        scale = jnp.zeros((slots, width), jnp.float32)
        for j in range(per):
            h = peer(k) * per + j
            base = pl.multiple_of(h * group, group)
            xs = jnp.concatenate([x[i, pl.ds(base, group), :] for i in range(latent // LANES)], axis=1)
            hi = xs.astype(jnp.bfloat16)
            lo = (xs - hi.astype(jnp.float32)).astype(jnp.bfloat16)
            both = jnp.dot(jnp.concatenate([hi, lo], axis=0), w[h], preferred_element_type=jnp.float32)
            part = both[:group] + both[group:]
            if k == 0:
                own[j] = part
            else:
                peak = jnp.maximum(jnp.max(jnp.abs(part), axis=1, keepdims=True), 1e-30)
                send[k, j] = jnp.round(part * (CODE / peak)).astype(jnp.int32).astype(jnp.int16)
                for t in range(toks):
                    scale = jnp.where(scale_lane == t * per + j, peak[t * slots:(t + 1) * slots], scale)
        if k != 0:
            top, den = stats_of(peer(k))
            meta_out[k, 0] = scale * (1.0 / CODE)
            meta_out[k, 1] = top
            meta_out[k, 2] = den
            if k == order[0]:
                pl.semaphore_wait(barrier, n - 1)
            meta_copy(k).start()
            rs_copy(k).start()

    tops, dens, scales = [], [], [None]
    top, den = stats_of(me)
    tops.append(top)
    dens.append(den)
    for k in range(1, n):
        meta_copy(k).wait_recv()
        scales.append(meta_in[k, 0])
        tops.append(meta_in[k, 1])
        dens.append(meta_in[k, 2])
    largest = functools.reduce(jnp.maximum, tops)
    factors = [jnp.exp(t - largest) for t in tops]
    total = functools.reduce(lambda a, b: a + b, [f * d for f, d in zip(factors, dens)])
    coefs = []
    for k in range(n):
        ratio = factors[k] / total
        if k:
            ratio = ratio * scales[k]
        coefs.append(jnp.concatenate(
            [pltpu.roll(ratio, width - t * per, 1) if t else ratio for t in range(toks)], axis=0))
    for k in order:
        rs_copy(k).wait_recv()
    for j in range(per):
        acc = own[j] * coefs[0][:, j:j + 1]
        for k in range(1, n):
            acc = acc + recv[k, j].astype(jnp.float32) * coefs[k][:, j:j + 1]
        if direct:
            turned[pl.ds(j, group, stride=per), :] = acc
        else:
            out_ref[me * per + j] = acc.astype(jnp.bfloat16)
    if direct:
        place = pl.multiple_of(me * per, per)
        for t in range(toks):
            for b in range(slots):
                row = (t * slots + b) * per
                out_ref[b * toks + t, pl.ds(place, per), :] = turned[row:row + per, :].astype(jnp.bfloat16)
    for k in order:
        ag_copy(k).start()
    for k in order:
        meta_copy(k).wait_send()
        rs_copy(k).wait_send()
    for k in order:
        ag_copy(k).wait()


def per_device(n, q_latent, q_rope, cache_latent, rope_keys, lengths, slot_request, value_up):
    toks, heads = q_latent.shape[1], q_latent.shape[2]
    slots, page, latent = cache_latent.shape
    dv = value_up.shape[2]
    group = toks * slots
    per = heads // n
    direct = per % 16 == 0
    rows = toks * heads
    width = -(-rows // LANES) * LANES
    hbm = pl.BlockSpec(memory_space=pltpu.HBM)
    smem = pl.BlockSpec(memory_space=pltpu.SMEM)
    dma = pltpu.SemaphoreType.DMA
    out = pl.pallas_call(
        functools.partial(kernel, n),
        out_shape=jax.ShapeDtypeStruct(
            (group, heads, dv) if direct else (heads, group, dv), jnp.bfloat16),
        in_specs=[smem, smem, hbm, hbm, hbm, hbm, hbm],
        out_specs=pl.BlockSpec(memory_space=pltpu.VMEM),
        scratch_shapes=[
            pltpu.VMEM(q_latent.shape, jnp.bfloat16),
            pltpu.VMEM(q_rope.shape, jnp.bfloat16),
            pltpu.VMEM(cache_latent.shape, jnp.bfloat16),
            pltpu.VMEM(rope_keys.shape, jnp.bfloat16),
            pltpu.VMEM(value_up.shape, jnp.bfloat16),
            pltpu.VMEM((slots, rows, page), jnp.bfloat16),
            pltpu.VMEM((latent // LANES, heads * group, LANES), jnp.float32),
            pltpu.VMEM((per, group, dv), jnp.float32),
            pltpu.VMEM((per * group, dv), jnp.float32),
            pltpu.VMEM((n, per, group, dv), jnp.int16),
            pltpu.VMEM((n, per, group, dv), jnp.int16),
            pltpu.VMEM((n, 3, slots, width), jnp.float32),
            pltpu.VMEM((n, 3, slots, width), jnp.float32),
            dma((4,)), dma((n,)), dma((n,)), dma((n,)), dma((n,)), dma((n,)), dma((n,)), dma((n,)),
        ],
        compiler_params=pltpu.CompilerParams(
            collective_id=0, has_side_effects=True, vmem_limit_bytes=67043328),
    )(lengths, slot_request, q_latent, q_rope, cache_latent, rope_keys, value_up)
    if direct:
        return out.reshape(slots, toks, heads, dv)
    return jnp.transpose(out.reshape(heads, toks, slots, dv), (2, 1, 0, 3))


def solution(mesh):
    in_specs = (
        P("groups", None, "head", None),
        P("groups", None, "head", None),
        P(("groups", "rep"), "seq", None),
        P(("groups", "rep"), None, "seq"),
        P(("groups", "rep")),
        P(("groups", "rep")),
        P("head", None, None),
    )
    out_specs = P(("groups", "rep"), None, "head", None)
    return jax.shard_map(
        functools.partial(per_device, mesh.shape["seq"]),
        mesh=mesh, in_specs=in_specs, out_specs=out_specs, check_vma=False,
    )
```

```python
import functools

import jax
import jax.numpy as jnp
from jax import lax
from jax.experimental import pallas as pl
from jax.experimental.pallas import tpu as pltpu
from jax.sharding import PartitionSpec as P

ROPE = 64
NOPE = 128
MESH = pl.DeviceIdType.MESH
LANES = 128
CODE = 32767.0


negative_fill = -1e30


def kernel(n, lengths_ref, request_ref, qlat_hbm, qrot_hbm, cache_hbm, rope_hbm, w_hbm, out_ref,
           qlat, qrot, cache, rope, w, weights, x, own, turned, send, recv, meta_out, meta_in,
           load_sem, w_sem, rs_ssem, rs_rsem, meta_ssem, meta_rsem, ag_ssem, ag_rsem):
    slots, page, latent = cache.shape
    toks, heads = qlat.shape[1], qlat.shape[2]
    rows = toks * heads
    group = toks * slots
    per = heads // n
    direct = per % 16 == 0
    me = lax.axis_index("seq")
    order = sorted(range(1, n), key=lambda k: abs(k - n / 2))

    def peer(k):
        return lax.rem(me + k, n)

    loads = [
        pltpu.make_async_copy(src, dst, load_sem.at[i])
        for i, (src, dst) in enumerate(
            ((qlat_hbm, qlat), (cache_hbm, cache), (qrot_hbm, qrot), (rope_hbm, rope)))
    ]
    for copy in loads:
        copy.start()

    def w_load(k):
        part = pl.ds(peer(k) * per, per)
        return pltpu.make_async_copy(w_hbm.at[part], w.at[part], w_sem.at[k])

    barrier = pltpu.get_barrier_semaphore()
    for k in order:
        pl.semaphore_signal(barrier, inc=1, device_id={"seq": peer(k)}, device_id_type=MESH)

    for copy in loads:
        copy.wait()
    for k in order + [0]:
        w_load(k).start()

    softmax_scale = (NOPE + ROPE) ** (-0.5)
    lane = lax.broadcasted_iota(jnp.int32, (rows, LANES), 1)
    token = lax.broadcasted_iota(jnp.int32, (rows, page), 0) // heads
    position = me * page + lax.broadcasted_iota(jnp.int32, (rows, page), 1)
    stat = jnp.zeros((rows, LANES), jnp.float32)
    for b in range(slots):
        r = request_ref[b]
        ql = qlat[r].reshape(rows, latent)
        qr = qrot[r].reshape(rows, qrot.shape[3])
        s = lax.dot_general(ql, cache[b], (((1,), (1,)), ((), ())), preferred_element_type=jnp.float32)
        s = s + jnp.dot(qr, rope[b], preferred_element_type=jnp.float32)
        s = s * softmax_scale
        visible = position < lengths_ref[b] - toks + 1 + token
        masked = jnp.where(visible, s, negative_fill)
        top = jnp.max(masked, axis=1, keepdims=True)
        e = jnp.where(visible, jnp.exp(masked - top), 0.0)
        den = jnp.sum(e, axis=1, keepdims=True)
        stat = jnp.where(lane == b, top, stat)
        stat = jnp.where(lane == slots + b, den, stat)
        weights[b] = e.astype(jnp.bfloat16)
    width = meta_out.shape[3]
    if rows < width:
        stat = jnp.concatenate([stat, jnp.zeros((width - rows, LANES), jnp.float32)], axis=0)
    mine = jnp.transpose(stat)[: 2 * slots]
    meta_lane = lax.broadcasted_iota(jnp.int32, (2 * slots, width), 1)
    scale_lane = meta_lane[:slots]

    def stats_of(dest):
        picked = mine
        for t in range(toks):
            shift = lax.rem(2 * width - t * (heads - per) - dest * per, width)
            moved = pltpu.roll(mine, shift, 1)
            picked = moved if t == 0 else jnp.where(meta_lane >= t * per, moved, picked)
        return picked[:slots], picked[slots:]

    def remote(src, dst, ssem, rsem, k):
        return pltpu.make_async_remote_copy(
            src_ref=src, dst_ref=dst, send_sem=ssem, recv_sem=rsem,
            device_id={"seq": peer(k)}, device_id_type=MESH)

    def rs_copy(k):
        return remote(send.at[k], recv.at[k], rs_ssem.at[k], rs_rsem.at[k], k)

    def meta_copy(k):
        return remote(meta_out.at[k], meta_in.at[k], meta_ssem.at[k], meta_rsem.at[k], k)

    def ag_copy(k):
        part = pl.ds(me * per, per)
        part = out_ref.at[:, part] if direct else out_ref.at[part]
        return remote(part, part, ag_ssem.at[k], ag_rsem.at[k], k)

    for b in range(slots):
        po = jnp.dot(weights[b], cache[b], preferred_element_type=jnp.float32)
        for t in range(toks):
            for i in range(latent // LANES):
                x[i, pl.ds(t * slots + b, heads, stride=group), :] = (
                    po[t * heads:(t + 1) * heads, i * LANES:(i + 1) * LANES])

    for k in order + [0]:
        w_load(k).wait()
        scale = jnp.zeros((slots, width), jnp.float32)
        for j in range(per):
            h = peer(k) * per + j
            base = pl.multiple_of(h * group, group)
            xs = jnp.concatenate([x[i, pl.ds(base, group), :] for i in range(latent // LANES)], axis=1)
            hi = xs.astype(jnp.bfloat16)
            lo = (xs - hi.astype(jnp.float32)).astype(jnp.bfloat16)
            both = jnp.dot(jnp.concatenate([hi, lo], axis=0), w[h], preferred_element_type=jnp.float32)
            part = both[:group] + both[group:]
            if k == 0:
                own[j] = part
            else:
                peak = jnp.maximum(jnp.max(jnp.abs(part), axis=1, keepdims=True), 1e-30)
                send[k, j] = jnp.round(part * (CODE / peak)).astype(jnp.int32).astype(jnp.int16)
                for t in range(toks):
                    scale = jnp.where(scale_lane == t * per + j, peak[t * slots:(t + 1) * slots], scale)
        if k != 0:
            top, den = stats_of(peer(k))
            meta_out[k, 0] = scale * (1.0 / CODE)
            meta_out[k, 1] = top
            meta_out[k, 2] = den
            if k == order[0]:
                pl.semaphore_wait(barrier, n - 1)
            meta_copy(k).start()
            rs_copy(k).start()

    tops, dens, scales = [], [], [None]
    top, den = stats_of(me)
    tops.append(top)
    dens.append(den)
    for k in range(1, n):
        meta_copy(k).wait_recv()
        scales.append(meta_in[k, 0])
        tops.append(meta_in[k, 1])
        dens.append(meta_in[k, 2])
    largest = functools.reduce(jnp.maximum, tops)
    factors = [jnp.exp(t - largest) for t in tops]
    total = functools.reduce(lambda a, b: a + b, [f * d for f, d in zip(factors, dens)])
    coefs = []
    for k in range(n):
        ratio = factors[k] / total
        if k:
            ratio = ratio * scales[k]
        coefs.append(jnp.concatenate(
            [pltpu.roll(ratio, width - t * per, 1) if t else ratio for t in range(toks)], axis=0))
    for k in order:
        rs_copy(k).wait_recv()
    for j in range(per):
        acc = own[j] * coefs[0][:, j:j + 1]
        for k in range(1, n):
            acc = acc + recv[k, j].astype(jnp.float32) * coefs[k][:, j:j + 1]
        if direct:
            turned[pl.ds(j, group, stride=per), :] = acc
        else:
            out_ref[me * per + j] = acc.astype(jnp.bfloat16)
    if direct:
        place = pl.multiple_of(me * per, per)
        for t in range(toks):
            for b in range(slots):
                row = (t * slots + b) * per
                out_ref[b * toks + t, pl.ds(place, per), :] = turned[row:row + per, :].astype(jnp.bfloat16)
    for k in order:
        ag_copy(k).start()
    for k in order:
        meta_copy(k).wait_send()
        rs_copy(k).wait_send()
    for k in order:
        ag_copy(k).wait()


def per_device(n, q_latent, q_rope, cache_latent, rope_keys, lengths, slot_request, value_up):
    toks, heads = q_latent.shape[1], q_latent.shape[2]
    slots, page, latent = cache_latent.shape
    dv = value_up.shape[2]
    group = toks * slots
    per = heads // n
    direct = per % 16 == 0
    rows = toks * heads
    width = -(-rows // LANES) * LANES
    hbm = pl.BlockSpec(memory_space=pltpu.HBM)
    smem = pl.BlockSpec(memory_space=pltpu.SMEM)
    dma = pltpu.SemaphoreType.DMA
    out = pl.pallas_call(
        functools.partial(kernel, n),
        out_shape=jax.ShapeDtypeStruct(
            (group, heads, dv) if direct else (heads, group, dv), jnp.bfloat16),
        in_specs=[smem, smem, hbm, hbm, hbm, hbm, hbm],
        out_specs=pl.BlockSpec(memory_space=pltpu.VMEM),
        scratch_shapes=[
            pltpu.VMEM(q_latent.shape, jnp.bfloat16),
            pltpu.VMEM(q_rope.shape, jnp.bfloat16),
            pltpu.VMEM(cache_latent.shape, jnp.bfloat16),
            pltpu.VMEM(rope_keys.shape, jnp.bfloat16),
            pltpu.VMEM(value_up.shape, jnp.bfloat16),
            pltpu.VMEM((slots, rows, page), jnp.bfloat16),
            pltpu.VMEM((latent // LANES, heads * group, LANES), jnp.float32),
            pltpu.VMEM((per, group, dv), jnp.float32),
            pltpu.VMEM((per * group, dv), jnp.float32),
            pltpu.VMEM((n, per, group, dv), jnp.int16),
            pltpu.VMEM((n, per, group, dv), jnp.int16),
            pltpu.VMEM((n, 3, slots, width), jnp.float32),
            pltpu.VMEM((n, 3, slots, width), jnp.float32),
            dma((4,)), dma((n,)), dma((n,)), dma((n,)), dma((n,)), dma((n,)), dma((n,)), dma((n,)),
        ],
        compiler_params=pltpu.CompilerParams(
            collective_id=0, has_side_effects=True, vmem_limit_bytes=67043328),
    )(lengths, slot_request, q_latent, q_rope, cache_latent, rope_keys, value_up)
    if direct:
        return out.reshape(slots, toks, heads, dv)
    return jnp.transpose(out.reshape(heads, toks, slots, dv), (2, 1, 0, 3))


def solution(mesh):
    in_specs = (
        P("groups", None, "head", None),
        P("groups", None, "head", None),
        P(("groups", "rep"), "seq", None),
        P(("groups", "rep"), None, "seq"),
        P(("groups", "rep")),
        P(("groups", "rep")),
        P("head", None, None),
    )
    out_specs = P(("groups", "rep"), None, "head", None)
    return jax.shard_map(
        functools.partial(per_device, mesh.shape["seq"]),
        mesh=mesh, in_specs=in_specs, out_specs=out_specs, check_vma=False,
    )
```
